32 devices in a mesh: rep: 1, dp: 32 (over x, y, z, core).
Axes of the slice: x: 2, y: 2, z: 4, core: 2. Of those that a mesh axis runs over, the one named last changes fastest.
Arguments:
- a: bfloat16 [32, 2, 4096, 1024], P(('rep', 'dp'))
- g: bfloat16 [32, 2, 4096, 4096], P(('rep', 'dp'))
Outputs:
- output: bfloat16 [2, 1024, 4096], P('rep')
All inputs are finite; a program needn't handle non-finite values.
Results may differ from the reference program's by a relative error of at most 0.012.
Values are sent between devices in bfloat16 or wider.
A program may use at most 2 GiB of HBM per device.

```python
import jax
import jax.numpy as jnp
from jax import lax

DEVICES = 32
MATRICES = 2
TOKENS = 4096
D = 1024
FF = 4096


def setup_inputs(seed: int = 0, part: int = 0) -> dict:
    ka, kg, ks = (jax.random.fold_in(k, part) for k in jax.random.split(jax.random.key(seed), 3))
    size = 2.0 ** jax.random.uniform(ks, (DEVICES, MATRICES, 1, 1), jnp.float32, -1.0, 1.0)
    a = jax.random.normal(ka, (DEVICES, MATRICES, TOKENS, D), jnp.float32)
    g = size * jax.random.normal(kg, (DEVICES, MATRICES, TOKENS, FF), jnp.float32) * (DEVICES * TOKENS) ** -0.5
    return {"a": a.astype(jnp.bfloat16), "g": g.astype(jnp.bfloat16)}


def reference(a, g):
    def take(so_far, one):
        return so_far + jnp.einsum("ntd,ntf->ndf", *one, preferred_element_type=jnp.float32), None

    return lax.scan(take, jnp.zeros((MATRICES, D, FF), jnp.float32), (a, g))[0].astype(jnp.bfloat16)
```

```python
import jax
import jax.numpy as jnp
from jax import lax
from jax.experimental import pallas as pl
from jax.experimental.pallas import tpu as pltpu
from jax.sharding import PartitionSpec as P

MESH = pl.DeviceIdType.MESH
TOKENS, D, FF, MATS = 4096, 1024, 4096, 2
COLS = 512
PER = FF // COLS
UNITS = MATS * PER
ROWS = (512, 256, 128, 64, 32)
LEVELS = 5
SEND_SLOTS = 4

REDUCE = ((1, 1, 0), (2, 2, 1), (3, 3, 2), (4, 4, 1), (5, 5, 1))
GATHER = ((6, 7, 3), (7, 8, 3), (8, 9, 3), (9, 10, 3))


TAIL = (
    (1, 15), (10, 0), (6, 5), (6, 6), (10, 1), (6, 7), (6, 8), (10, 2), (6, 9), (2, 14), (4, 12), (3, 13),
    (7, 4), (5, 11), (6, 10), (9, 3), (3, 14), (10, 3), (2, 15), (5, 12), (7, 5), (7, 6), (8, 4), (7, 7),
    (7, 8), (7, 9), (6, 11), (4, 13), (7, 10), (3, 15), (4, 14), (6, 12), (9, 4), (8, 5), (7, 11), (10, 4),
    (7, 12), (8, 6), (9, 5), (8, 7), (10, 5), (9, 6), (8, 8), (10, 6), (9, 7), (8, 9), (10, 7), (5, 13),
    (4, 15), (9, 8), (8, 10), (10, 8), (5, 14), (9, 9), (10, 9), (8, 11), (9, 10), (8, 12), (10, 10), (6, 13),
    (5, 15), (9, 11), (6, 14), (10, 11), (9, 12), (7, 13), (6, 15), (7, 14), (10, 12), (7, 15), (8, 13), (8, 14),
    (9, 13), (8, 15), (10, 13), (9, 14), (10, 14), (9, 15), (10, 15),
)


def kernel(a_ref, g_ref, o_ref, a_v, g_v, p_v, k1, k2, k3, k4, s0, s1, s2, s3, s4, r0, r1, r2, r3, r4,
           a_sem, g_sem, send_sem, recv_sem):
    me = lax.axis_index("dp")
    x, y, z, c = me // 16, (me // 8) % 2, (me // 2) % 4, me % 2
    zl, zh = z % 2, z // 2

    def at(x, y, z, c):
        return ((x * 2 + y) * 4 + z) * 2 + c

    first = at(x * c + (1 - x) * (1 - c), y * (1 - c) + (1 - y) * c, z, c)
    second = at(x * (1 - c) + (1 - x) * c, y * c + (1 - y) * (1 - c), z, c)
    partner = (at(x, y, z, 1 - c), first, at(x, y, z + 1 - 2 * zl, c), second, at(x, y, z + 2 - 4 * zh, c))
    bit = (c, x * (1 - c) + y * c, zl, y * (1 - c) + x * c, zh)
    base = [0]
    for lvl in range(LEVELS):
        base.append(base[-1] + bit[lvl] * ROWS[lvl])

    stage = (s0, s1, s2, s3, s4)
    recv = (r0, r1, r2, r3, r4)
    keep = (None, k1, k2, k3, k4)

    def remote(src, dst, lvl, s, u):
        return pltpu.make_async_remote_copy(
            src, dst, send_sem.at[s, u % SEND_SLOTS], recv_sem.at[s, u],
            device_id=(0, partner[lvl]), device_id_type=MESH)

    def reduce_copy(lvl, u):
        return remote(stage[lvl].at[u % 2], recv[lvl].at[u], lvl, lvl, u)

    def out_at(u, row, rows):
        col = pl.multiple_of((u % PER) * COLS, COLS)
        return (u // PER, pl.ds(pl.multiple_of(row, 32), rows), pl.ds(col, COLS))

    def gather_copy(lvl, u):
        where = o_ref.at[out_at(u, base[lvl + 1], ROWS[lvl])]
        return remote(where, where, lvl, 9 - lvl, u)

    def when(cond, fn):
        if cond is True:
            fn()
        elif cond is not False:
            pl.when(cond)(fn)

    def reduce_stage(lvl, u):
        reduce_copy(lvl - 1, u).wait_recv()
        got, rows = recv[lvl - 1].at[u], ROWS[lvl - 1]
        half = rows // 2
        if lvl < LEVELS:
            when(u >= 2, lambda: reduce_copy(lvl, u - 2).wait_send())
            go = pl.multiple_of((1 - bit[lvl]) * half, half)
            st = pl.multiple_of(bit[lvl] * half, half)
            if lvl == 1:
                out, mine = p_v[u % 2, 0], p_v[u % 2, 1]
            else:
                held = keep[lvl - 1].at[u % 2]
                out, mine = held[pl.ds(go, half)], held[pl.ds(st, half)]
            stage[lvl][u % 2] = (out + got[pl.ds(go, half)].astype(jnp.float32)).astype(jnp.bfloat16)
            keep[lvl][u % 2] = mine + got[pl.ds(st, half)].astype(jnp.float32)
            reduce_copy(lvl, u).start()
        else:
            total = keep[lvl - 1][u % 2] + got[...].astype(jnp.float32)
            o_ref[out_at(u, base[LEVELS], rows)] = total.astype(jnp.bfloat16)
            when(u >= SEND_SLOTS, lambda: gather_copy(LEVELS - 1, u - SEND_SLOTS).wait_send())
            gather_copy(LEVELS - 1, u).start()

    def gather_stage(s, u):
        lvl = 10 - s
        gather_copy(lvl, u).wait_recv()
        if lvl > 0:
            when(u >= SEND_SLOTS, lambda: gather_copy(lvl - 1, u - SEND_SLOTS).wait_send())
            gather_copy(lvl - 1, u).start()

    def run(s, u):
        reduce_stage(s, u) if s <= LEVELS else gather_stage(s, u)

    def a_copy(m, d):
        col = pl.multiple_of(d * 256, 256)
        return pltpu.make_async_copy(a_ref.at[0, m, :, pl.ds(col, 256)], a_v.at[d], a_sem.at[d])

    def g_copy(u):
        col = pl.multiple_of((u % PER) * COLS, COLS)
        return pltpu.make_async_copy(g_ref.at[0, u // PER, :, pl.ds(col, COLS)], g_v.at[u % 2], g_sem.at[u % 2])

    block = (2 * (1 - c), 2 * (1 - c) + 1, 2 * c + 1 - bit[1], 2 * c + bit[1])

    a_copy(0, block[0]).start()
    g_copy(0).start()
    for j in range(1, 4):
        a_copy(0, block[j]).start()

    barrier = pltpu.get_barrier_semaphore()
    for p in partner:
        pl.semaphore_signal(barrier, inc=1, device_id=(0, p), device_id_type=MESH)
    pl.semaphore_wait(barrier, LEVELS)

    @pl.loop(0, UNITS)
    def _(t):
        pl.when(t + 1 < UNITS)(lambda: g_copy(t + 1).start())
        g_copy(t).wait()
        m = t // PER
        for j in range(4):
            pl.when(t % PER == 0)(lambda: a_copy(m, block[j]).wait())
            if j == 0:
                pl.when(t >= 2)(lambda: reduce_copy(0, t - 2).wait_send())
            r = lax.dot_general(a_v[block[j]], g_v[t % 2], (((0,), (0,)), ((), ())),
                                preferred_element_type=jnp.float32)
            if j < 2:
                s0[t % 2, j * 256:(j + 1) * 256] = r.astype(jnp.bfloat16)
            else:
                p_v[t % 2, j - 2] = r
            pl.when(t == PER - 1)(lambda: a_copy(1, block[j]).start())
            if j == 1:
                reduce_copy(0, t).start()
            for s, lag, gap in REDUCE:
                if gap == j:
                    pl.when(t >= lag)(lambda: run(s, t - lag))
            for s, off, gap in GATHER:
                if gap == j:
                    pl.when((t >= off) & ((t - off) % 2 == 0))(lambda: run(s, (t - off) // 2))

    for s, u in TAIL:
        run(s, u)
    for lvl in range(LEVELS):
        for u in range(UNITS - 2, UNITS):
            reduce_copy(lvl, u).wait_send()
        for u in range(UNITS - SEND_SLOTS, UNITS):
            gather_copy(lvl, u).wait_send()


def solution(mesh):
    def body(a, g):
        f32, bf16 = jnp.float32, jnp.bfloat16
        return pl.pallas_call(
            kernel,
            out_shape=pltpu.VMEM((MATS, D, FF), bf16),
            in_specs=[pl.BlockSpec(memory_space=pl.ANY)] * 2,
            out_specs=pl.BlockSpec(memory_space=pltpu.VMEM),
            scratch_shapes=[
                pltpu.VMEM((4, TOKENS, 256), bf16),
                pltpu.VMEM((2, TOKENS, COLS), bf16),
                pltpu.VMEM((2, 2, 256, COLS), f32),
                *(pltpu.VMEM((2, rows, COLS), f32) for rows in ROWS[1:]),
                *(pltpu.VMEM((2, rows, COLS), bf16) for rows in ROWS),
                *(pltpu.VMEM((UNITS, rows, COLS), bf16) for rows in ROWS),
                pltpu.SemaphoreType.DMA((4,)),
                pltpu.SemaphoreType.DMA((2,)),
                pltpu.SemaphoreType.DMA((10, SEND_SLOTS)),
                pltpu.SemaphoreType.DMA((10, UNITS)),
            ],
            compiler_params=pltpu.CompilerParams(
                collective_id=0, has_side_effects=True, vmem_limit_bytes=47 * 2**20),
            cost_estimate=pl.CostEstimate(flops=2 * MATS * TOKENS * D * FF, bytes_accessed=84 * 2**20, transcendentals=0),
            name="sum_units",
        )(a, g)

    every = P(("rep", "dp"))
    return jax.shard_map(body, mesh=mesh, in_specs=(every, every), out_specs=P("rep"), check_vma=False)
```

```python
import jax
import jax.numpy as jnp
from jax import lax
from jax.experimental import pallas as pl
from jax.experimental.pallas import tpu as pltpu
from jax.sharding import PartitionSpec as P

MESH = pl.DeviceIdType.MESH
TOKENS, D, FF, MATS = 4096, 1024, 4096, 2
COLS = 512
PER = FF // COLS
UNITS = MATS * PER
ROWS = (512, 256, 128, 64, 32)
LEVELS = 5
STAGE_SLOTS = 2
SEND_SLOTS = 8

REDUCE = (3, 7, 13, 16, 22)
GATHER, RATE = (25, 29, 40, 51), 5
TAIL = (
    (3, 13), (10, 0), (6, 8), (10, 1), (8, 5), (9, 3), (6, 9), (7, 7), (10, 2), (9, 4), (10, 3), (8, 6),
    (4, 12), (10, 4), (5, 11), (6, 10), (2, 15), (4, 13), (3, 14), (7, 8), (8, 7), (9, 5), (7, 9), (5, 12),
    (10, 5), (6, 11), (9, 6), (3, 15), (7, 10), (4, 14), (10, 6), (5, 13), (8, 8), (9, 7), (7, 11), (4, 15),
    (10, 7), (8, 9), (6, 12), (9, 8), (8, 10), (10, 8), (5, 14), (9, 9), (6, 13), (7, 12), (10, 9), (8, 11),
    (9, 10), (5, 15), (7, 13), (6, 14), (10, 10), (8, 12), (9, 11), (6, 15), (7, 14), (10, 11), (8, 13), (9, 12),
    (7, 15), (8, 14), (10, 12), (9, 13), (10, 13), (8, 15), (9, 14), (10, 14), (9, 15), (10, 15),
)


def kernel(a_ref, g_ref, o_ref, a_v, g_v, p_v, k1, k2, k3, k4, s0, s1, s2, s3, s4, r0, r1, r2, r3, r4,
           a_sem, g_sem, send_sem, recv_sem):
    me = lax.axis_index("dp")
    x, y, z, c = me // 16, (me // 8) % 2, (me // 2) % 4, me % 2
    zl, zh = z % 2, z // 2

    def at(x, y, z, c):
        return ((x * 2 + y) * 4 + z) * 2 + c

    first = at(x * c + (1 - x) * (1 - c), y * (1 - c) + (1 - y) * c, z, c)
    second = at(x * (1 - c) + (1 - x) * c, y * c + (1 - y) * (1 - c), z, c)
    partner = (at(x, y, z, 1 - c), first, at(x, y, z + 1 - 2 * zl, c), second, at(x, y, z + 2 - 4 * zh, c))
    bit = (c, x * (1 - c) + y * c, zl, y * (1 - c) + x * c, zh)
    base = [0]
    for lvl in range(LEVELS):
        base.append(base[-1] + bit[lvl] * ROWS[lvl])

    stage = (s0, s1, s2, s3, s4)
    recv = (r0, r1, r2, r3, r4)
    keep = (None, k1, k2, k3, k4)

    def remote(src, dst, lvl, s, u):
        return pltpu.make_async_remote_copy(
            src, dst, send_sem.at[s, u % SEND_SLOTS], recv_sem.at[s, u],
            device_id=(0, partner[lvl]), device_id_type=MESH)

    def reduce_copy(lvl, u):
        return remote(stage[lvl].at[u % STAGE_SLOTS], recv[lvl].at[u], lvl, lvl, u)

    def out_at(u, row, rows):
        col = pl.multiple_of((u % PER) * COLS, COLS)
        return (u // PER, pl.ds(pl.multiple_of(row, 32), rows), pl.ds(col, COLS))

    def gather_copy(lvl, u):
        where = o_ref.at[out_at(u, base[lvl + 1], ROWS[lvl])]
        return remote(where, where, lvl, 9 - lvl, u)

    def when(cond, fn):
        if cond is True:
            fn()
        elif cond is not False:
            pl.when(cond)(fn)

    def reduce_stage(lvl, u):
        reduce_copy(lvl - 1, u).wait_recv()
        got, rows = recv[lvl - 1].at[u], ROWS[lvl - 1]
        half = rows // 2
        if lvl < LEVELS:
            when(u >= STAGE_SLOTS, lambda: reduce_copy(lvl, u - STAGE_SLOTS).wait_send())
            go = pl.multiple_of((1 - bit[lvl]) * half, half)
            st = pl.multiple_of(bit[lvl] * half, half)
            if lvl == 1:
                out, mine = p_v[u % 2, 0], p_v[u % 2, 1]
            else:
                held = keep[lvl - 1].at[u % 2]
                out, mine = held[pl.ds(go, half)], held[pl.ds(st, half)]
            stage[lvl][u % STAGE_SLOTS] = (out + got[pl.ds(go, half)].astype(jnp.float32)).astype(jnp.bfloat16)
            keep[lvl][u % 2] = mine + got[pl.ds(st, half)].astype(jnp.float32)
            reduce_copy(lvl, u).start()
        else:
            total = keep[lvl - 1][u % 2] + got[...].astype(jnp.float32)
            o_ref[out_at(u, base[LEVELS], rows)] = total.astype(jnp.bfloat16)
            when(u >= SEND_SLOTS, lambda: gather_copy(LEVELS - 1, u - SEND_SLOTS).wait_send())
            gather_copy(LEVELS - 1, u).start()

    def gather_stage(s, u):
        lvl = 10 - s
        gather_copy(lvl, u).wait_recv()
        if lvl > 0:
            when(u >= SEND_SLOTS, lambda: gather_copy(lvl - 1, u - SEND_SLOTS).wait_send())
            gather_copy(lvl - 1, u).start()

    def run(s, u):
        reduce_stage(s, u) if s <= LEVELS else gather_stage(s, u)

    def a_copy(m, d):
        col = pl.multiple_of(d * 256, 256)
        return pltpu.make_async_copy(a_ref.at[0, m, :, pl.ds(col, 256)], a_v.at[d], a_sem.at[d])

    def g_copy(u):
        col = pl.multiple_of((u % PER) * COLS, COLS)
        return pltpu.make_async_copy(g_ref.at[0, u // PER, :, pl.ds(col, COLS)], g_v.at[u % 2], g_sem.at[u % 2])

    block = (2 * (1 - c), 2 * (1 - c) + 1, 2 * c + 1 - bit[1], 2 * c + bit[1])

    a_copy(0, block[0]).start()
    g_copy(0).start()
    for j in range(1, 4):
        a_copy(0, block[j]).start()

    barrier = pltpu.get_barrier_semaphore()
    for p in partner:
        pl.semaphore_signal(barrier, inc=1, device_id=(0, p), device_id_type=MESH)
    pl.semaphore_wait(barrier, LEVELS)

    @pl.loop(0, UNITS)
    def _(t):
        pl.when(t + 1 < UNITS)(lambda: g_copy(t + 1).start())
        g_copy(t).wait()
        m = t // PER
        for j in range(4):
            pl.when(t % PER == 0)(lambda: a_copy(m, block[j]).wait())
            if j == 0:
                pl.when(t >= STAGE_SLOTS)(lambda: reduce_copy(0, t - STAGE_SLOTS).wait_send())
            r = lax.dot_general(a_v[block[j]], g_v[t % 2], (((0,), (0,)), ((), ())),
                                preferred_element_type=jnp.float32)
            if j < 2:
                s0[t % STAGE_SLOTS, j * 256:(j + 1) * 256] = r.astype(jnp.bfloat16)
            else:
                p_v[t % 2, j - 2] = r
            pl.when(t == PER - 1)(lambda: a_copy(1, block[j]).start())
            if j == 1:
                reduce_copy(0, t).start()
            i = 4 * t + j
            for s, at_block in enumerate(REDUCE, 1):
                if at_block % 4 == j:
                    pl.when(t >= at_block // 4)(lambda: run(s, t - at_block // 4))
            for s, at_block in enumerate(GATHER, 6):
                due = i - at_block
                if RATE != 4:
                    pl.when((due >= 0) & (lax.rem(due + 8 * RATE * 4, RATE) == 0))(lambda: run(s, due // RATE))
                elif at_block % 4 == j:
                    pl.when(t >= at_block // 4)(lambda: run(s, t - at_block // 4))

    for s, u in TAIL:
        run(s, u)
    for lvl in range(LEVELS):
        for u in range(UNITS - STAGE_SLOTS, UNITS):
            reduce_copy(lvl, u).wait_send()
        for u in range(UNITS - SEND_SLOTS, UNITS):
            gather_copy(lvl, u).wait_send()


def solution(mesh):
    def body(a, g):
        f32, bf16 = jnp.float32, jnp.bfloat16
        return pl.pallas_call(
            kernel,
            out_shape=pltpu.VMEM((MATS, D, FF), bf16),
            in_specs=[pl.BlockSpec(memory_space=pl.ANY)] * 2,
            out_specs=pl.BlockSpec(memory_space=pltpu.VMEM),
            scratch_shapes=[
                pltpu.VMEM((4, TOKENS, 256), bf16),
                pltpu.VMEM((2, TOKENS, COLS), bf16),
                pltpu.VMEM((2, 2, 256, COLS), f32),
                *(pltpu.VMEM((2, rows, COLS), f32) for rows in ROWS[1:]),
                *(pltpu.VMEM((STAGE_SLOTS, rows, COLS), bf16) for rows in ROWS),
                *(pltpu.VMEM((UNITS, rows, COLS), bf16) for rows in ROWS),
                pltpu.SemaphoreType.DMA((4,)),
                pltpu.SemaphoreType.DMA((2,)),
                pltpu.SemaphoreType.DMA((10, SEND_SLOTS)),
                pltpu.SemaphoreType.DMA((10, UNITS)),
            ],
            compiler_params=pltpu.CompilerParams(
                collective_id=0, has_side_effects=True, vmem_limit_bytes=47 * 2**20),
            cost_estimate=pl.CostEstimate(flops=2 * MATS * TOKENS * D * FF, bytes_accessed=84 * 2**20, transcendentals=0),
            name="sum_units",
        )(a, g)

    every = P(("rep", "dp"))
    return jax.shard_map(body, mesh=mesh, in_specs=(every, every), out_specs=P("rep"), check_vma=False)
```

```python
import jax
import jax.numpy as jnp
from jax import lax
from jax.experimental import pallas as pl
from jax.experimental.pallas import tpu as pltpu
from jax.sharding import PartitionSpec as P

MESH = pl.DeviceIdType.MESH
TOKENS, D, FF, MATS = 4096, 1024, 4096, 2
COLS = 512
PER = FF // COLS
UNITS = MATS * PER
ROWS = (512, 256, 128, 64, 32)
LEVELS = 5
STAGE_SLOTS = 4
SEND_SLOTS = 16

REDUCE = (3, 7, 13, 17, 21)
GATHER, RATE = (25, 27, 33, 47), 4
TAIL = (
    (4, 12), (3, 13), (10, 0), (10, 1), (10, 2), (9, 5), (10, 3), (9, 6), (8, 8), (5, 11), (10, 4), (9, 7),
    (6, 10), (10, 5), (10, 6), (3, 14), (10, 7), (2, 15), (4, 13), (8, 9), (9, 8), (5, 12), (7, 10), (6, 11),
    (4, 14), (10, 8), (3, 15), (9, 9), (5, 13), (7, 11), (6, 12), (4, 15), (10, 9), (8, 10), (5, 14), (7, 12),
    (6, 13), (8, 11), (9, 10), (5, 15), (7, 13), (6, 14), (10, 10), (8, 12), (9, 11), (6, 15), (7, 14), (10, 11),
    (8, 13), (9, 12), (7, 15), (10, 12), (8, 14), (9, 13), (10, 13), (8, 15), (9, 14), (10, 14), (9, 15), (10, 15),
)


def kernel(a_ref, g_ref, o_ref, a_v, g_v, p_v, k1, k2, k3, k4, s0, s1, s2, s3, s4, r0, r1, r2, r3, r4,
           a_sem, g_sem, send_sem, recv_sem):
    me = lax.axis_index("dp")
    x, y, z, c = me // 16, (me // 8) % 2, (me // 2) % 4, me % 2
    zl, zh = z % 2, z // 2

    def at(x, y, z, c):
        return ((x * 2 + y) * 4 + z) * 2 + c

    first = at(x * c + (1 - x) * (1 - c), y * (1 - c) + (1 - y) * c, z, c)
    second = at(x * (1 - c) + (1 - x) * c, y * c + (1 - y) * (1 - c), z, c)
    partner = (at(x, y, z, 1 - c), first, at(x, y, z + 1 - 2 * zl, c), second, at(x, y, z + 2 - 4 * zh, c))
    bit = (c, x * (1 - c) + y * c, zl, y * (1 - c) + x * c, zh)
    base = [0]
    for lvl in range(LEVELS):
        base.append(base[-1] + bit[lvl] * ROWS[lvl])

    stage = (s0, s1, s2, s3, s4)
    recv = (r0, r1, r2, r3, r4)
    keep = (None, k1, k2, k3, k4)

    def remote(src, dst, lvl, s, u):
        return pltpu.make_async_remote_copy(
            src, dst, send_sem.at[s, u % SEND_SLOTS], recv_sem.at[s, u],
            device_id=(0, partner[lvl]), device_id_type=MESH)

    def reduce_copy(lvl, u):
        return remote(stage[lvl].at[u % STAGE_SLOTS], recv[lvl].at[u], lvl, lvl, u)

    def out_at(u, row, rows):
        col = pl.multiple_of((u % PER) * COLS, COLS)
        return (u // PER, pl.ds(pl.multiple_of(row, 32), rows), pl.ds(col, COLS))

    def gather_copy(lvl, u):
        where = o_ref.at[out_at(u, base[lvl + 1], ROWS[lvl])]
        return remote(where, where, lvl, 9 - lvl, u)

    def when(cond, fn):
        if cond is True:
            fn()
        elif cond is not False:
            pl.when(cond)(fn)

    def reduce_stage(lvl, u):
        reduce_copy(lvl - 1, u).wait_recv()
        got, rows = recv[lvl - 1].at[u], ROWS[lvl - 1]
        half = rows // 2
        if lvl < LEVELS:
            when(u >= STAGE_SLOTS, lambda: reduce_copy(lvl, u - STAGE_SLOTS).wait_send())
            go = pl.multiple_of((1 - bit[lvl]) * half, half)
            st = pl.multiple_of(bit[lvl] * half, half)
            if lvl == 1:
                out, mine = p_v[u % 2, 0], p_v[u % 2, 1]
            else:
                held = keep[lvl - 1].at[u % 2]
                out, mine = held[pl.ds(go, half)], held[pl.ds(st, half)]
            stage[lvl][u % STAGE_SLOTS] = (out + got[pl.ds(go, half)].astype(jnp.float32)).astype(jnp.bfloat16)
            keep[lvl][u % 2] = mine + got[pl.ds(st, half)].astype(jnp.float32)
            reduce_copy(lvl, u).start()
        else:
            total = keep[lvl - 1][u % 2] + got[...].astype(jnp.float32)
            o_ref[out_at(u, base[LEVELS], rows)] = total.astype(jnp.bfloat16)
            when(u >= SEND_SLOTS, lambda: gather_copy(LEVELS - 1, u - SEND_SLOTS).wait_send())
            gather_copy(LEVELS - 1, u).start()

    def gather_stage(s, u):
        lvl = 10 - s
        gather_copy(lvl, u).wait_recv()
        if lvl > 0:
            when(u >= SEND_SLOTS, lambda: gather_copy(lvl - 1, u - SEND_SLOTS).wait_send())
            gather_copy(lvl - 1, u).start()

    def run(s, u):
        reduce_stage(s, u) if s <= LEVELS else gather_stage(s, u)

    def a_copy(m, d):
        col = pl.multiple_of(d * 256, 256)
        return pltpu.make_async_copy(a_ref.at[0, m, :, pl.ds(col, 256)], a_v.at[d], a_sem.at[d])

    def g_copy(u):
        col = pl.multiple_of((u % PER) * COLS, COLS)
        return pltpu.make_async_copy(g_ref.at[0, u // PER, :, pl.ds(col, COLS)], g_v.at[u % 2], g_sem.at[u % 2])

    block = (2 * (1 - c), 2 * (1 - c) + 1, 2 * c + 1 - bit[1], 2 * c + bit[1])

    a_copy(0, block[0]).start()
    g_copy(0).start()
    for j in range(1, 4):
        a_copy(0, block[j]).start()

    barrier = pltpu.get_barrier_semaphore()
    for p in partner:
        pl.semaphore_signal(barrier, inc=1, device_id=(0, p), device_id_type=MESH)
    pl.semaphore_wait(barrier, LEVELS)

    @pl.loop(0, UNITS)
    def _(t):
        pl.when(t + 1 < UNITS)(lambda: g_copy(t + 1).start())
        g_copy(t).wait()
        m = t // PER
        for j in range(4):
            if j % 2 == 0:
                @pl.when(t % PER == 0)
                def _():
                    a_copy(m, block[j]).wait()
                    a_copy(m, block[j + 1]).wait()

            if j == 0:
                pl.when(t >= STAGE_SLOTS)(lambda: reduce_copy(0, t - STAGE_SLOTS).wait_send())
            r = lax.dot_general(a_v[block[j]], g_v[t % 2], (((0,), (0,)), ((), ())),
                                preferred_element_type=jnp.float32)
            if j < 2:
                s0[t % STAGE_SLOTS, j * 256:(j + 1) * 256] = r.astype(jnp.bfloat16)
            else:
                p_v[t % 2, j - 2] = r
            if j % 2 == 0:
                continue

            @pl.when(t == PER - 1)
            def _():
                a_copy(1, block[j - 1]).start()
                a_copy(1, block[j]).start()

            if j == 1:
                reduce_copy(0, t).start()
            i = 4 * t + j
            for s, at_block in enumerate(REDUCE, 1):
                if at_block % 4 == j:
                    pl.when(t >= at_block // 4)(lambda: run(s, t - at_block // 4))
            for s, at_block in enumerate(GATHER, 6):
                due = i - at_block
                if RATE != 4:
                    pl.when((due >= 0) & (lax.rem(due + 8 * RATE * 4, RATE) == 0))(lambda: run(s, due // RATE))
                elif at_block % 4 == j:
                    pl.when(t >= at_block // 4)(lambda: run(s, t - at_block // 4))

    for s, u in TAIL:
        run(s, u)
    for lvl in range(LEVELS):
        for u in range(UNITS - STAGE_SLOTS, UNITS):
            reduce_copy(lvl, u).wait_send()
        for u in range(UNITS - SEND_SLOTS, UNITS):
            gather_copy(lvl, u).wait_send()


def solution(mesh):
    def body(a, g):
        f32, bf16 = jnp.float32, jnp.bfloat16
        return pl.pallas_call(
            kernel,
            out_shape=pltpu.VMEM((MATS, D, FF), bf16),
            in_specs=[pl.BlockSpec(memory_space=pl.ANY)] * 2,
            out_specs=pl.BlockSpec(memory_space=pltpu.VMEM),
            scratch_shapes=[
                pltpu.VMEM((4, TOKENS, 256), bf16),
                pltpu.VMEM((2, TOKENS, COLS), bf16),
                pltpu.VMEM((2, 2, 256, COLS), f32),
                *(pltpu.VMEM((2, rows, COLS), f32) for rows in ROWS[1:]),
                *(pltpu.VMEM((STAGE_SLOTS, rows, COLS), bf16) for rows in ROWS),
                *(pltpu.VMEM((UNITS, rows, COLS), bf16) for rows in ROWS),
                pltpu.SemaphoreType.DMA((4,)),
                pltpu.SemaphoreType.DMA((2,)),
                pltpu.SemaphoreType.DMA((10, SEND_SLOTS)),
                pltpu.SemaphoreType.DMA((10, UNITS)),
            ],
            compiler_params=pltpu.CompilerParams(
                collective_id=0, has_side_effects=True, vmem_limit_bytes=47 * 2**20),
            cost_estimate=pl.CostEstimate(flops=2 * MATS * TOKENS * D * FF, bytes_accessed=84 * 2**20, transcendentals=0),
            name="sum_units",
        )(a, g)

    every = P(("rep", "dp"))
    return jax.shard_map(body, mesh=mesh, in_specs=(every, every), out_specs=P("rep"), check_vma=False)
```
